32 devices in a mesh: dp: 16 (over z, y, core), seq: 2 (over x).
Axes of the slice: x: 2, y: 2, z: 4, core: 2. Of those that a mesh axis runs over, the one named last changes fastest.
Arguments:
- fields: bfloat16 [16, 1024, 276], P('dp', 'seq'), may hold values from -6 to 6
- targets: float32 [16, 1024, 276], P('dp', 'seq'), may hold values from -6 to 6
- counts: int32 [16, 5], P('dp'), may hold values from 5 to 13
- lead_step: int32 [16], P('dp'), may hold values from 0 to 7
- step_count: int32 [], replicated, may hold values from 2 to 20
- attention_mats: float32 [4, 384, 384], P(None, 'dp')
- attention_mom: float32 [4, 384, 384], P(None, 'dp'), may hold values from -3.33786e-06 to 3.33786e-06
- feedforward_mats: float32 [2, 384, 1536], P(None, 'dp'), may hold values from -0.3125 to 0.3125
- feedforward_mom: float32 [2, 384, 1536], P(None, 'dp'), may hold values from -3.33786e-06 to 3.33786e-06
- modulation_mat: float32 [384, 2304], P('dp'), may hold values from -0.3125 to 0.3125
- modulation_first: float32 [384, 2304], P('dp'), may hold values from -3.5762787e-07 to 3.5762787e-07
- modulation_second: float32 [384, 2304], P('dp'), may hold values from 1.65e-14 to 6.6e-14
- pooling_mats: float32 [2, 384, 384], P(None, 'dp'), may hold values from -0.625 to 0.625
- pooling_first: float32 [2, 384, 384], P(None, 'dp'), may hold values from -3.5762787e-07 to 3.5762787e-07
- pooling_second: float32 [2, 384, 384], P(None, 'dp'), may hold values from 1.65e-14 to 6.6e-14
- lookup_table: float32 [641, 384], P(None, 'dp')
- table_first: float32 [641, 384], P(None, 'dp'), may hold values from -3.5762787e-07 to 3.5762787e-07
- table_second: float32 [641, 384], P(None, 'dp'), may hold values from 1.65e-14 to 6.6e-14
Outputs:
- loss: float32 [], replicated
- grad_norm: float32 [], replicated
- attention_new: float32 [4, 384, 384], P(None, 'dp')
- attention_fresh: float32 [4, 384, 384], P(None, 'dp')
- feedforward_new: float32 [2, 384, 1536], P(None, 'dp')
- feedforward_fresh: float32 [2, 384, 1536], P(None, 'dp')
- modulation_new: float32 [384, 2304], P('dp')
- modulation_first_new: float32 [384, 2304], P('dp')
- modulation_second_new: float32 [384, 2304], P('dp')
- pooling_new: float32 [2, 384, 384], P(None, 'dp')
- pooling_first_new: float32 [2, 384, 384], P(None, 'dp')
- pooling_second_new: float32 [2, 384, 384], P(None, 'dp')
- table_new: float32 [641, 384], P(None, 'dp')
- table_first_new: float32 [641, 384], P(None, 'dp')
- table_second_new: float32 [641, 384], P(None, 'dp')
The draws below stay inside these ranges and needn't reach their ends.
Inputs may be any that keep to these rules, and one draw needn't show every extreme that they name: Levels 0 to counts - 1 of each atmospheric variable are present, the others missing.
All inputs are finite; a program needn't handle non-finite values.
Results may differ from the reference program's by a relative error of at most 0.0097.
Values may be sent and summed in bfloat16 or wider, within the bound.
A program may use at most 128 MiB of HBM per device.

```python
import math
import jax
import jax.numpy as jnp
from jax import lax

D = 384
HEADS = 6
FF = 1536
SURF = 4
GROUPS = 5
LEVELS = 13
PATCH_PIX = 4
NLEAD = 8
PCOLS = 128
VARS = 69
SEQLEN = 1024
ITEMS = 16
ROWS = 641


def base_draw(key, shape):
    return jax.random.normal(key, shape, jnp.float32)


def draw_attention_mats(key, part):
    base = base_draw(key, (4, D, D))
    scales = jnp.array([0.8, 0.8, 1.0, 0.6 * math.sqrt(SEQLEN)], jnp.float32) / math.sqrt(D)
    return base * scales[:, None, None]


def draw_lookup_table(key, part):
    width_in = VARS * PATCH_PIX
    count = 2 * width_in + VARS + NLEAD + HEADS + 6
    scales = jnp.concatenate([jnp.full((width_in,), 0.5, jnp.float32), jnp.full((VARS,), 0.5, jnp.float32), jnp.full((NLEAD,), 1.0, jnp.float32), jnp.full((HEADS,), 2.0, jnp.float32), jnp.full((6,), 1.0, jnp.float32), jnp.full((width_in,), 1.0 / math.sqrt(D), jnp.float32)])
    return base_draw(key, (count, D)) * scales[:, None]


def plant(entries, stream_key, smallest, largest):
    dims = entries.shape
    spot = [jax.random.randint(jax.random.fold_in(stream_key, axis), (), 0, dims[axis]) for axis in range(len(dims))]
    entries = entries.at[tuple(spot)].set(smallest)
    longest = dims.index(max(dims))
    spot[longest] = (spot[longest] + 1) % dims[longest]
    return entries.at[tuple(spot)].set(largest)


def shard_levels(rng, dims, shards, least, largest):
    gain, own = 1.0, jax.random.fold_in(rng, 6)
    for dim, shards_of in shards:
        heights = jnp.exp(jax.random.uniform(jax.random.fold_in(own, dim), (shards_of,), jnp.float32, least / len(shards), largest / len(shards)))
        gain = gain * jnp.repeat(heights, dims[dim] // shards_of).reshape([-1 if axis == dim else 1 for axis in range(len(dims))])
    return gain


def bell_draw(own_key, shape, scale, most, shards=(), kind=jnp.bfloat16):
    gain = shard_levels(own_key, shape, shards, -0.22, 0.18) if shards else 1.0
    drawn = jax.random.normal(own_key, shape, jnp.float32) * scale * gain
    return jnp.minimum(jnp.maximum(drawn, -most), most).astype(kind)


def setup_inputs(seed: int = 0) -> dict:
    streams_of = jax.random.split(jax.random.key(seed), 19)
    return {
        "fields": bell_draw(streams_of[0], (ITEMS, SEQLEN, VARS * PATCH_PIX), 1.0, 6.0, ((0, 16), (1, 2))),
        "targets": bell_draw(streams_of[1], (ITEMS, SEQLEN, VARS * PATCH_PIX), 1.0, 6.0, ((0, 16), (1, 2)), jnp.float32),
        "counts": plant(jax.random.randint(streams_of[2], (ITEMS, GROUPS), LEVELS - 8, LEVELS + 1), jax.random.fold_in(streams_of[2], 1), LEVELS - 8, LEVELS).astype(jnp.int32),
        "lead_step": plant(jax.random.randint(streams_of[3], (ITEMS,), 0, NLEAD), jax.random.fold_in(streams_of[3], 1), 0, NLEAD - 1).astype(jnp.int32),
        "step_count": jax.random.randint(streams_of[4], (), 2, 21).astype(jnp.int32),
        "attention_mats": draw_attention_mats(jax.random.fold_in(streams_of[18], 71), 0),
        "attention_mom": bell_draw(streams_of[6], (4, D, D), (5.6e-7), 3.337860107421875e-06, ((1, 16),), jnp.float32),
        "feedforward_mats": bell_draw(streams_of[7], (2, D, FF), D ** -0.5, 0.3125, ((1, 16),), jnp.float32),
        "feedforward_mom": bell_draw(streams_of[8], (2, D, FF), (5.6e-7), 3.337860107421875e-06, ((1, 16),), jnp.float32),
        "modulation_mat": bell_draw(streams_of[9], (D, 6 * D), D ** -0.5, 0.3125, ((0, 16),), jnp.float32),
        "modulation_first": bell_draw(streams_of[10], (D, 6 * D), (6.2e-8), 3.5762786865234375e-07, ((0, 16),), jnp.float32),
        "modulation_second": jnp.clip(jnp.exp(math.log(6.60000008746893e-14) - 1.3862944 * jax.random.uniform(streams_of[11], (D, 6 * D), jnp.float32) ** shard_levels(streams_of[11], (D, 6 * D), ((0, 16),), -0.2, 0.2)), 1.6500000218672324e-14, 6.60000008746893e-14),
        "pooling_mats": bell_draw(streams_of[12], (2, D, D), (D // 4) ** -0.5, 0.625, ((1, 16),), jnp.float32),
        "pooling_first": bell_draw(streams_of[13], (2, D, D), (6.2e-8), 3.5762786865234375e-07, ((1, 16),), jnp.float32),
        "pooling_second": jnp.clip(jnp.exp(math.log(6.60000008746893e-14) - 1.3862944 * jax.random.uniform(streams_of[14], (2, D, D), jnp.float32) ** shard_levels(streams_of[14], (2, D, D), ((1, 16),), -0.2, 0.2)), 1.6500000218672324e-14, 6.60000008746893e-14),
        "lookup_table": draw_lookup_table(jax.random.fold_in(streams_of[18], 71), 0),
        "table_first": bell_draw(streams_of[16], (ROWS, D), (6.2e-8), 3.5762786865234375e-07, ((1, 16),), jnp.float32),
        "table_second": jnp.clip(jnp.exp(math.log(6.60000008746893e-14) - 1.3862944 * jax.random.uniform(streams_of[17], (ROWS, D), jnp.float32) ** shard_levels(streams_of[17], (ROWS, D), ((1, 16),), -0.2, 0.2)), 1.6500000218672324e-14, 6.60000008746893e-14),
    }


norm_eps = 1e-06
clip_limit = 0.001
muon_mu = 0.95
muon_rate = 0.6
muon_decay = 0.01
adam_rate = 0.05
adam_one = 0.9
adam_two = 0.95
adam_eps = 1e-08
adam_decay = 0.1
ns_a = 3.4445
ns_b = -4.775
ns_c = 2.0315
mask_fill = -1000000000.0
highest = lax.Precision.HIGHEST

@jax.custom_vjp
def low(v):
    return lax.optimization_barrier(v.astype(jnp.bfloat16)).astype(jnp.float32)

@jax.custom_vjp
def low_back(v):
    return v

def low_keep(v):
    return (low(v), None)

def low_pass(kept, grad):
    return (grad,)

def back_keep(v):
    return (v, None)

def back_low(kept, grad):
    return (low(grad),)
low.defvjp(low_keep, low_pass)
low_back.defvjp(back_keep, back_low)

def high_dot(a, b):
    return jnp.dot(a, b, precision=highest, preferred_element_type=jnp.float32)

def layer_norm(values):
    average = lax.optimization_barrier(jnp.mean(values, axis=-1, keepdims=True))
    centered = values - average
    return centered * lax.rsqrt(lax.optimization_barrier(jnp.mean(centered * centered, axis=-1, keepdims=True)) + norm_eps)

def offsets():
    width_in = VARS * PATCH_PIX
    lead_at = width_in + VARS
    query_at = lead_at + NLEAD
    bias_at = query_at + HEADS
    head_at = bias_at + 6
    return (width_in, lead_at, query_at, bias_at, head_at)

def presence(count_row):
    levels = jnp.arange(LEVELS, dtype=jnp.int32)
    table_grid = (levels[None, :] < count_row[:, None]).astype(jnp.float32).reshape(-1)
    return jnp.concatenate([jnp.ones((SURF,), jnp.float32), table_grid])

def lat_weight(first_row, count, grid_rows):
    patch = first_row + jnp.arange(count, dtype=jnp.int32)
    pix_row = 2 * (patch // PCOLS)[:, None] + (jnp.arange(PATCH_PIX, dtype=jnp.int32) // 2)[None, :]
    angle = ((pix_row.astype(jnp.float32) + 0.5) / grid_rows - 0.5) * math.pi
    return jnp.cos(angle)

def aggregate(lookup, value_w, out_w, pix_rows, present):
    width_in, lead_at, query_at, bias_at, head_at = offsets()
    count = pix_rows.shape[0]
    embedding = lookup[:width_in].reshape(VARS, PATCH_PIX, D)
    var_bias = lookup[width_in:lead_at]
    pool_query = lookup[query_at:bias_at]
    key_embed = jnp.einsum('vpd,hd->vph', embedding, pool_query, precision=highest) / math.sqrt(D)
    key_bias = jnp.einsum('vd,hd->hv', var_bias, pool_query, precision=highest) / math.sqrt(D)
    val_embed = jnp.einsum('vpd,dc->vpc', embedding, value_w, precision=highest).reshape(VARS, PATCH_PIX, HEADS, D // HEADS)
    val_bias = high_dot(var_bias, value_w).reshape(VARS, HEADS, D // HEADS)
    pixels = pix_rows.reshape(count, VARS, PATCH_PIX)
    scores = jnp.einsum('nvp,vph->nhv', pixels, key_embed, precision=highest) + key_bias[None]
    scores = jnp.where(present[None, None, :] > 0.5, scores, mask_fill)
    mixing = jax.nn.softmax(scores, axis=-1)
    spread = mixing[:, :, :, None] * pixels[:, None, :, :]
    pooled = jnp.einsum('nhvp,vphc->nhc', spread, val_embed, precision=highest)
    pooled = pooled + jnp.einsum('nhv,vhc->nhc', mixing, val_bias, precision=highest)
    return high_dot(pooled.reshape(count, D), out_w)

def modulation(lookup, mod_mat, lead_index):
    width_in, lead_at, query_at, bias_at, head_at = offsets()
    lead_row = lax.dynamic_index_in_dim(lookup, lead_at + lead_index, 0, keepdims=False)
    condition = jax.nn.silu(lead_row)
    return high_dot(condition[None, :], mod_mat).reshape(6, D) + lookup[bias_at:head_at]

def attention(queries, keys, values):
    length = queries.shape[0]
    block = math.gcd(512, length)
    head_dim = D // HEADS
    scale = 1.0 / math.sqrt(head_dim)
    key_heads = keys.reshape(length, HEADS, head_dim)
    value_heads = values.reshape(length, HEADS, head_dim)

    def one_block(query_block):
        scores = low_back(jnp.einsum('qhc,khc->hqk', query_block, key_heads, precision=highest) * scale)
        log_total = jax.nn.logsumexp(scores, axis=-1, keepdims=True)
        probs = jnp.exp(scores - log_total)
        return low_back(jnp.einsum('hqk,khc->qhc', low(probs), value_heads, precision=highest))
    blocks = queries.reshape(length // block, block, HEADS, head_dim)
    return lax.map(jax.checkpoint(one_block), blocks).reshape(length, D)

def item_loss(weights, lat, item):
    attention_b, feed_b, mod_b, pool_b, lookup_b = weights
    fields_item, targets_item, count_row, lead_index = item
    width_in, lead_at, query_at, bias_at, head_at = offsets()
    length = fields_item.shape[0]
    present = presence(count_row)
    stream_in = aggregate(lookup_b, pool_b[0], pool_b[1], fields_item, present)
    modul = modulation(lookup_b, mod_b, lead_index)
    entry = layer_norm(stream_in) * (1.0 + modul[1]) + modul[0]
    joined = jnp.concatenate([attention_b[0], attention_b[1], attention_b[2]], axis=1)
    triple = low_back(high_dot(low(entry), joined))
    queries = low(triple[:, :D])
    keys = low(triple[:, D:2 * D])
    values = low(triple[:, 2 * D:])
    attended = attention(queries, keys, values)
    branch = low_back(high_dot(low(attended), attention_b[3]))
    stream_mid = stream_in + modul[2] * branch
    inner = layer_norm(stream_mid) * (1.0 + modul[4]) + modul[3]
    upper = low_back(high_dot(low(inner), feed_b[0]))
    lowered = low_back(high_dot(low(jax.nn.gelu(upper)), feed_b[1].T))
    stream_out = stream_mid + modul[5] * lowered
    final = layer_norm(stream_out)
    pred = low_back(high_dot(low(final), lookup_b[head_at:].T))
    weight = (lat[:, None, :] * present[None, :, None]).reshape(length, width_in)
    miss = pred - targets_item
    return jnp.sum(weight * miss * miss)

def orthogonalize(matrix):
    current = matrix / (jnp.sqrt(jnp.sum(matrix * matrix)) + 1e-07)
    for sweep in range(5):
        gram = high_dot(current, current.T)
        polynomial = ns_b * gram + ns_c * high_dot(gram, gram)
        current = ns_a * current + high_dot(polynomial, current)
    return current

def muon(weight, momentum, gradient):
    fresh = muon_mu * momentum + gradient
    orthogonal = jax.vmap(orthogonalize)(fresh)
    return (weight * (1.0 - muon_rate * muon_decay) - muon_rate * orthogonal, fresh)

def adamw(weight, first, second, gradient, step_count):
    first_new = adam_one * first + (1.0 - adam_one) * gradient
    second_new = adam_two * second + (1.0 - adam_two) * gradient * gradient
    steps_done = step_count.astype(jnp.float32)
    first_hat = first_new / (1.0 - adam_one ** steps_done)
    second_hat = second_new / (1.0 - adam_two ** steps_done)
    weight_new = weight - adam_rate * (first_hat / (jnp.sqrt(second_hat) + adam_eps) + adam_decay * weight)
    return (weight_new, first_new, second_new)

def reference(fields, targets, counts, lead_step, step_count, attention_mats, attention_mom, feedforward_mats, feedforward_mom, modulation_mat, modulation_first, modulation_second, pooling_mats, pooling_first, pooling_second, lookup_table, table_first, table_second):
    grid_rows = 2 * SEQLEN // PCOLS
    lat = lat_weight(0, SEQLEN, grid_rows)
    present_all = jax.vmap(presence)(counts)
    weight_total = jnp.sum(lat) * jnp.sum(present_all)
    fields_f = fields.astype(jnp.float32)
    params = (attention_mats, feedforward_mats, modulation_mat, pooling_mats, lookup_table)

    def total_loss(params):
        rounded = jax.tree.map(low, params)

        def one_item(item):
            return item_loss(rounded, lat, item)
        sums = lax.map(jax.checkpoint(one_item), (fields_f, targets, counts, lead_step))
        return jnp.sum(sums) / weight_total
    loss, pull = jax.vjp(total_loss, params)
    grads = pull(jnp.ones_like(loss))[0]
    square = jnp.float32(0.0)
    for gradient in grads:
        square = square + jnp.sum(gradient * gradient)
    grad_norm = jnp.sqrt(square)
    factor = clip_limit / jnp.maximum(grad_norm, clip_limit)
    clipped = [gradient * factor for gradient in grads]
    attention_new, attention_fresh = muon(attention_mats, attention_mom, clipped[0])
    feedforward_new, feedforward_fresh = muon(feedforward_mats, feedforward_mom, clipped[1])
    modulation_new, modulation_first_new, modulation_second_new = adamw(modulation_mat, modulation_first, modulation_second, clipped[2], step_count)
    pooling_new, pooling_first_new, pooling_second_new = adamw(pooling_mats, pooling_first, pooling_second, clipped[3], step_count)
    table_new, table_first_new, table_second_new = adamw(lookup_table, table_first, table_second, clipped[4], step_count)
    return (loss, grad_norm, attention_new, attention_fresh, feedforward_new, feedforward_fresh, modulation_new, modulation_first_new, modulation_second_new, pooling_new, pooling_first_new, pooling_second_new, table_new, table_first_new, table_second_new)
```

```python
import math

import jax
import jax.numpy as jnp
from jax import lax
from jax.sharding import PartitionSpec as P

D = 384
HEADS = 6
SURF = 4
LEVELS = 13
PATCH_PIX = 4
NLEAD = 8
PCOLS = 128
VARS = 69


norm_eps = 1e-06
clip_limit = 0.001
muon_mu = 0.95
muon_rate = 0.6
muon_decay = 0.01
adam_rate = 0.05
adam_one = 0.9
adam_two = 0.95
adam_eps = 1e-08
adam_decay = 0.1
ns_a = 3.4445
ns_b = -4.775
ns_c = 2.0315
mask_fill = -1000000000.0
highest = lax.Precision.HIGHEST


def high_dot(a, b):
    return jnp.dot(a, b, precision=highest, preferred_element_type=jnp.float32)


def plain_dot(a, b):
    return jnp.dot(a, b, preferred_element_type=jnp.float32)


def contract_last(a, b):
    return lax.dot_general(a, b, (((1,), (1,)), ((), ())), preferred_element_type=jnp.float32)


def contract_first(a, b):
    return lax.dot_general(a, b, (((0,), (0,)), ((), ())), preferred_element_type=jnp.float32)


def layer_norm(values):
    average = jnp.mean(values, axis=-1, keepdims=True)
    centered = values - average
    return centered * lax.rsqrt(jnp.mean(centered * centered, axis=-1, keepdims=True) + norm_eps)


def offsets():
    width_in = VARS * PATCH_PIX
    lead_at = width_in + VARS
    query_at = lead_at + NLEAD
    bias_at = query_at + HEADS
    head_at = bias_at + 6
    return (width_in, lead_at, query_at, bias_at, head_at)


def presence(count_row):
    levels = jnp.arange(LEVELS, dtype=jnp.int32)
    table_grid = (levels[None, :] < count_row[:, None]).astype(jnp.float32).reshape(-1)
    return jnp.concatenate([jnp.ones((SURF,), jnp.float32), table_grid])


def lat_weight(first_row, count, grid_rows):
    patch = first_row + jnp.arange(count, dtype=jnp.int32)
    pix_row = 2 * (patch // PCOLS)[:, None] + (jnp.arange(PATCH_PIX, dtype=jnp.int32) // 2)[None, :]
    angle = ((pix_row.astype(jnp.float32) + 0.5) / grid_rows - 0.5) * math.pi
    return jnp.cos(angle)


def aggregate(lookup, value_w, out_w, pix_rows, present):
    width_in, lead_at, query_at, bias_at, head_at = offsets()
    count = pix_rows.shape[0]
    head_dim = D // HEADS
    embedding = lookup[:width_in]
    var_bias = lookup[width_in:lead_at]
    pool_query = lookup[query_at:bias_at]
    select = (
        (jnp.arange(width_in, dtype=jnp.int32) // PATCH_PIX)[:, None]
        == jnp.arange(VARS, dtype=jnp.int32)[None, :]
    ).astype(jnp.float32)
    key_embed = contract_last_high(embedding, pool_query) / math.sqrt(D)
    key_block = (key_embed[:, :, None] * select[:, None, :]).reshape(width_in, HEADS * VARS)
    key_bias = contract_last_high(pool_query, var_bias) / math.sqrt(D)
    val_embed = high_dot(embedding, value_w).reshape(width_in, HEADS, head_dim)
    val_bias = high_dot(var_bias, value_w).reshape(VARS, HEADS, head_dim)
    scores = high_dot(pix_rows, key_block).reshape(count, HEADS, VARS) + key_bias[None]
    scores = jnp.where(present[None, None, :] > 0.5, scores, mask_fill)
    mixing = jax.nn.softmax(scores, axis=-1)
    repeated = high_dot(mixing.reshape(count * HEADS, VARS), select.T).reshape(
        count, HEADS, width_in
    )
    spread = repeated * pix_rows[:, None, :]
    pooled = jnp.einsum("nhk,khc->nhc", spread, val_embed, precision=highest)
    pooled = pooled + jnp.einsum("nhv,vhc->nhc", mixing, val_bias, precision=highest)
    return high_dot(pooled.reshape(count, D), out_w)


def contract_last_high(a, b):
    return lax.dot_general(
        a, b, (((1,), (1,)), ((), ())), precision=highest, preferred_element_type=jnp.float32
    )


def modulation(lookup, mod_mat, lead_index):
    width_in, lead_at, query_at, bias_at, head_at = offsets()
    lead_row = lax.dynamic_index_in_dim(lookup, lead_at + lead_index, 0, keepdims=False)
    condition = jax.nn.silu(lead_row)
    return high_dot(condition[None, :], mod_mat).reshape(6, D) + lookup[bias_at:head_at]


def entry_fn(stream, modul):
    return layer_norm(stream) * (1.0 + modul[1]) + modul[0]


def middle_fn(stream, modul, branch):
    stream_mid = stream + modul[2] * branch
    return (stream_mid, layer_norm(stream_mid) * (1.0 + modul[4]) + modul[3])


def closing_fn(stream, modul, lowered):
    return layer_norm(stream + modul[5] * lowered)


def orthogonalize(matrix):
    current = matrix / (jnp.sqrt(jnp.sum(matrix * matrix)) + 1e-07)
    for sweep in range(5):
        gram = high_dot(current, current.T)
        polynomial = ns_b * gram + ns_c * high_dot(gram, gram)
        current = ns_a * current + high_dot(polynomial, current)
    return current


def adamw(weight, first, second, gradient, step_count):
    first_new = adam_one * first + (1.0 - adam_one) * gradient
    second_new = adam_two * second + (1.0 - adam_two) * gradient * gradient
    steps_done = step_count.astype(jnp.float32)
    first_hat = first_new / (1.0 - adam_one**steps_done)
    second_hat = second_new / (1.0 - adam_two**steps_done)
    weight_new = weight - adam_rate * (
        first_hat / (jnp.sqrt(second_hat) + adam_eps) + adam_decay * weight
    )
    return (weight_new, first_new, second_new)


def split_high(a):
    upper = a.astype(jnp.bfloat16)
    return upper, (a - upper.astype(jnp.float32)).astype(jnp.bfloat16)


def mid_dot(a, b):
    return jnp.dot(a, b, precision=lax.Precision.HIGH, preferred_element_type=jnp.float32)


def orth_square(matrix):
    current = matrix / (jnp.sqrt(jnp.sum(matrix * matrix)) + 1e-07)
    for sweep in range(5):
        gram = mid_dot(current, current.T)
        polynomial = ns_b * gram + ns_c * mid_dot(gram, gram)
        current = ns_a * current + mid_dot(polynomial, current)
    return current


def orth_wide(matrix):
    start = matrix / (jnp.sqrt(jnp.sum(matrix * matrix)) + 1e-07)
    gram = mid_dot(start, start.T)
    eye = jnp.eye(matrix.shape[0], dtype=jnp.float32)
    product = None
    for sweep in range(5):
        polynomial = ns_a * eye + ns_b * gram + ns_c * mid_dot(gram, gram)
        product = polynomial if product is None else mid_dot(polynomial, product)
        if sweep < 4:
            gram = mid_dot(mid_dot(polynomial, gram), polynomial)
    return mid_dot(product, start)


def body(
    fields,
    targets,
    counts,
    lead_step,
    step_count,
    attention_mats,
    attention_mom,
    feedforward_mats,
    feedforward_mom,
    modulation_mat,
    modulation_first,
    modulation_second,
    pooling_mats,
    pooling_first,
    pooling_second,
    lookup_table,
    table_first,
    table_second,
):
    seq_count = lax.axis_size("seq")
    data_count = lax.axis_size("dp")
    rows = fields.shape[1]
    length = rows * seq_count
    head_dim = D // HEADS
    scale = 1.0 / math.sqrt(head_dim)
    width_in, lead_at, query_at, bias_at, head_at = offsets()
    own = attention_mats.shape[1]
    place = lax.axis_index("dp")
    here = lax.axis_index("seq")
    table_own = lookup_table.T.astype(jnp.bfloat16)
    lookup_t = lax.all_gather(table_own, "dp", axis=0, tiled=True)
    pool_b = lax.all_gather(pooling_mats.astype(jnp.bfloat16), "dp", axis=1, tiled=True)
    attention_b = lax.all_gather(attention_mats.astype(jnp.bfloat16), "dp", axis=1, tiled=True)
    feed_b = lax.all_gather(feedforward_mats.astype(jnp.bfloat16), "dp", axis=1, tiled=True)
    present = presence(counts[0])
    mod_own = modulation_mat.astype(jnp.bfloat16).astype(jnp.float32)
    lead_own = table_own[:, lead_at:query_at].astype(jnp.float32)
    cond_own, cond_back = jax.vjp(jax.nn.silu, lead_own)
    lead_part = lax.dot_general(
        cond_own, mod_own, (((0,), (0,)), ((), ())), precision=highest,
        preferred_element_type=jnp.float32,
    )
    count_row = jnp.full((1, 6 * D), jnp.sum(present), jnp.float32)
    lead_all = lax.psum(jnp.concatenate([lead_part, count_row]), "dp")
    bias_rows = lookup_t[:, bias_at:head_at].T.astype(jnp.float32)
    lead_hot = (jnp.arange(NLEAD, dtype=jnp.int32) == lead_step[0]).astype(jnp.float32)
    modul = (
        jnp.sum(lead_hot[:, None] * lead_all[:NLEAD], axis=0).reshape(6, D) + bias_rows
    )
    first_row = here * rows
    lat = lat_weight(first_row, rows, 2 * length // PCOLS)
    lat_all = lat_weight(0, length, 2 * length // PCOLS)
    weight = (lat[:, None, :] * present[None, :, None]).reshape(rows, width_in)
    weight_total = jnp.sum(lat_all) * lead_all[NLEAD, 0]
    pix_rows = fields[0].astype(jnp.float32)

    def prelude(lookup_f, pool_f):
        return aggregate(lookup_f.T, pool_f[0], pool_f[1], pix_rows, present)

    stream_in, prelude_back = jax.vjp(
        prelude, lookup_t.astype(jnp.float32), pool_b.astype(jnp.float32)
    )
    entry, entry_back = jax.vjp(entry_fn, stream_in, modul)
    entry_b = entry.astype(jnp.bfloat16)
    entry_all = lax.all_gather(entry_b, "seq", axis=0, tiled=True)
    queries = plain_dot(entry_b, attention_b[0]).astype(jnp.bfloat16)
    keys = plain_dot(entry_all, attention_b[1]).astype(jnp.bfloat16)
    values = plain_dot(entry_all, attention_b[2]).astype(jnp.bfloat16)
    queries_h = queries.reshape(rows, HEADS, head_dim)
    keys_h = keys.reshape(length, HEADS, head_dim)
    values_h = values.reshape(length, HEADS, head_dim)
    scores = (
        jnp.einsum("qhc,khc->hqk", queries_h, keys_h, preferred_element_type=jnp.float32) * scale
    )
    top = jnp.max(scores, axis=-1, keepdims=True)
    log_total = top + jnp.log(jnp.sum(jnp.exp(scores - top), axis=-1, keepdims=True))
    probs = jnp.exp(scores - log_total)
    probs_b = probs.astype(jnp.bfloat16)
    attended = jnp.einsum("hqk,khc->qhc", probs_b, values_h, preferred_element_type=jnp.float32)
    attended_b = attended.reshape(rows, D).astype(jnp.bfloat16)
    branch = plain_dot(attended_b, attention_b[3])
    (stream_mid, inner), middle_back = jax.vjp(middle_fn, stream_in, modul, branch)
    inner_b = inner.astype(jnp.bfloat16)
    upper = plain_dot(inner_b, feed_b[0])
    hidden, gelu_back = jax.vjp(jax.nn.gelu, upper)
    hidden_b = hidden.astype(jnp.bfloat16)
    lowered = contract_last(hidden_b, feed_b[1])
    final, closing_back = jax.vjp(closing_fn, stream_mid, modul, lowered)
    final_b = final.astype(jnp.bfloat16)
    head_t = lookup_t[:, head_at:]
    pred = plain_dot(final_b, head_t)
    miss = pred - targets[0]
    loss_part = jnp.sum(weight * miss * miss)
    dpred_b = (2.0 * weight * miss / weight_total).astype(jnp.bfloat16)
    dfinal = contract_last(dpred_b, head_t)
    dhead_t = contract_first(final_b, dpred_b)
    dstream_c, dmodul_c, dlowered = closing_back(dfinal)
    dlowered_b = dlowered.astype(jnp.bfloat16)
    dhidden = plain_dot(dlowered_b, feed_b[1])
    ddown = contract_first(dlowered_b, hidden_b)
    dupper_b = gelu_back(dhidden)[0].astype(jnp.bfloat16)
    dinner = contract_last(dupper_b, feed_b[0])
    dup = contract_first(inner_b, dupper_b)
    dstream_m, dmodul_m, dbranch = middle_back((dstream_c, dinner))
    dbranch_b = dbranch.astype(jnp.bfloat16)
    dattended_b = contract_last(dbranch_b, attention_b[3]).astype(jnp.bfloat16)
    dattended_h = dattended_b.reshape(rows, HEADS, head_dim)
    dout_w = contract_first(attended_b, dbranch_b)
    dprobs = jnp.einsum("qhc,khc->hqk", dattended_h, values_h, preferred_element_type=jnp.float32)
    delta = jnp.sum(probs * dprobs, axis=-1, keepdims=True)
    dscores_b = (probs * (dprobs - delta)).astype(jnp.bfloat16)
    dqueries = (
        jnp.einsum("hqk,khc->qhc", dscores_b, keys_h, preferred_element_type=jnp.float32) * scale
    )
    dkeys = (
        jnp.einsum("hqk,qhc->khc", dscores_b, queries_h, preferred_element_type=jnp.float32) * scale
    )
    dvalues = jnp.einsum("hqk,qhc->khc", probs_b, dattended_h, preferred_element_type=jnp.float32)
    dqueries_b = dqueries.reshape(rows, D).astype(jnp.bfloat16)
    dkeys_b = dkeys.reshape(length, D).astype(jnp.bfloat16)
    dvalues_b = dvalues.reshape(length, D).astype(jnp.bfloat16)
    dentry_all = contract_last(dkeys_b, attention_b[1]) + contract_last(dvalues_b, attention_b[2])
    dentry_far = lax.psum_scatter(
        dentry_all.astype(jnp.bfloat16), "seq", scatter_dimension=0, tiled=True
    )
    dentry = contract_last(dqueries_b, attention_b[0]) + dentry_far.astype(jnp.float32)
    dquery_w = contract_first(entry_b, dqueries_b)
    dkey_w = contract_first(entry_all, dkeys_b)
    dvalue_w = contract_first(entry_all, dvalues_b)
    dstream_e, dmodul_e = entry_back(dentry)
    dlookup_t, dpool = prelude_back(dstream_m + dstream_e)
    dmodul = dmodul_c + dmodul_m + dmodul_e
    dlead = lax.psum(lead_hot[:, None] * dmodul.reshape(1, 6 * D), ("dp", "seq"))
    dlookup_t = dlookup_t + jnp.pad(dhead_t, ((0, 0), (head_at, 0)))
    packed = jnp.concatenate(
        [dup, ddown, dquery_w, dkey_w, dvalue_w, dout_w, dpool[0], dpool[1],
         jnp.pad(dlookup_t, ((0, 0), (0, 2 * D - dlookup_t.shape[1])))],
        axis=1,
    ).astype(jnp.bfloat16)
    share = lax.psum(
        lax.psum_scatter(packed, "dp", scatter_dimension=0, tiled=True), "seq"
    ).astype(jnp.float32)
    wide = feedforward_mats.shape[2]
    feed_share = jnp.stack([share[:, :wide], share[:, wide : 2 * wide]])
    base = 2 * wide
    attention_share = jnp.stack([share[:, base + D * k : base + D * (k + 1)] for k in range(4)])
    pool_share = jnp.stack([share[:, base + D * k : base + D * (k + 1)] for k in (4, 5)])
    table_share = share[:, base + 6 * D : base + 6 * D + lookup_table.shape[0]]
    mod_share = high_dot(cond_own, dlead)
    dcond = lax.dot_general(
        mod_own, dlead, (((1,), (1,)), ((), ())), precision=highest,
        preferred_element_type=jnp.float32,
    )
    dlead_own = cond_back(dcond)[0]
    dbias = jnp.sum(dlead, axis=0).reshape(6, D).T
    dbias_own = lax.dynamic_slice_in_dim(dbias, place * own, own, 0)
    table_share = table_share + jnp.pad(
        jnp.concatenate([dlead_own, jnp.zeros((own, HEADS), jnp.float32), dbias_own], axis=1),
        ((0, 0), (lead_at, lookup_table.shape[0] - head_at)),
    )
    shares = (attention_share, feed_share, mod_share, pool_share, table_share)
    square_part = jnp.float32(0.0)
    for part in shares:
        square_part = square_part + jnp.sum(part * part)
    sums = lax.psum(jnp.stack([square_part / seq_count, loss_part]), ("dp", "seq"))
    loss = sums[1] / weight_total
    grad_norm = jnp.sqrt(sums[0])
    factor = clip_limit / jnp.maximum(grad_norm, clip_limit)
    clipped = [part * factor for part in shares]
    clipped[4] = clipped[4].T
    attention_fresh = muon_mu * attention_mom + clipped[0]
    feedforward_fresh = muon_mu * feedforward_mom + clipped[1]
    whole_attention, whole_feed = (
        lax.all_gather(attention_fresh.astype(jnp.bfloat16), "dp", axis=1, tiled=True),
        lax.all_gather(feedforward_fresh.astype(jnp.bfloat16), "dp", axis=1, tiled=True),
    )
    row_start = place * own
    attention_orth = lax.dynamic_slice_in_dim(
        jax.vmap(orth_square)(whole_attention.astype(jnp.float32)), row_start, own, 1
    )
    feed_orth = lax.dynamic_slice_in_dim(
        jax.vmap(orth_wide)(whole_feed.astype(jnp.float32)), row_start, own, 1
    )
    attention_new = attention_mats * (1.0 - muon_rate * muon_decay) - muon_rate * attention_orth
    feedforward_new = feedforward_mats * (1.0 - muon_rate * muon_decay) - muon_rate * feed_orth
    modulation_new, modulation_first_new, modulation_second_new = adamw(
        modulation_mat, modulation_first, modulation_second, clipped[2], step_count
    )
    pooling_new, pooling_first_new, pooling_second_new = adamw(
        pooling_mats, pooling_first, pooling_second, clipped[3], step_count
    )
    table_new, table_first_new, table_second_new = adamw(
        lookup_table, table_first, table_second, clipped[4], step_count
    )
    return (
        loss,
        grad_norm,
        attention_new,
        attention_fresh,
        feedforward_new,
        feedforward_fresh,
        modulation_new,
        modulation_first_new,
        modulation_second_new,
        pooling_new,
        pooling_first_new,
        pooling_second_new,
        table_new,
        table_first_new,
        table_second_new,
    )


def solution(mesh):
    placed = (
        P("dp", "seq", None),
        P("dp", "seq", None),
        P("dp", None),
        P("dp"),
        P(),
        P(None, "dp", None),
        P(None, "dp", None),
        P(None, "dp", None),
        P(None, "dp", None),
        P("dp", None),
        P("dp", None),
        P("dp", None),
        P(None, "dp", None),
        P(None, "dp", None),
        P(None, "dp", None),
        P(None, "dp"),
        P(None, "dp"),
        P(None, "dp"),
    )
    return jax.shard_map(
        body,
        mesh=mesh,
        in_specs=placed,
        out_specs=(
            P(),
            P(),
            P(None, "dp", None),
            P(None, "dp", None),
            P(None, "dp", None),
            P(None, "dp", None),
            P("dp", None),
            P("dp", None),
            P("dp", None),
            P(None, "dp", None),
            P(None, "dp", None),
            P(None, "dp", None),
            P(None, "dp"),
            P(None, "dp"),
            P(None, "dp"),
        ),
        check_vma=False,
    )
```
